256 devices in a mesh: tok: 32 (over z, y), head: 4 (over x), grp: 2 (over core).
Axes of the slice: x: 4, y: 4, z: 8, core: 2. Of those that a mesh axis runs over, the one named last changes fastest.
Arguments:
- tokens: bfloat16 [16384, 4096], P('tok', ('head', 'grp')), may hold values from -6 to 6
- norm_gain: bfloat16 [4096], P(('head', 'grp')), may hold values from 1.2 to 9, as said below
- query_key_value_weight: bfloat16 [4096, 6144], P(None, ('head', 'grp')), may hold values from -0.09375 to 0.09375
- out_weight: bfloat16 [4096, 4096], P(('head', 'grp')), may hold values from -0.09375 to 0.09375
- doc_ids: int32 [16384], P('tok'), may hold values from 0 to 15, never falling along the last dimension, each value on 1 to 8192 neighbouring positions
Outputs:
- attended: bfloat16 [16384, 4096], P('tok', ('head', 'grp'))
The draws below stay inside these ranges and needn't reach their ends.
Inputs may be any that keep to these rules, and one draw needn't show every extreme that they name: `norm_gain`: norm gains are positive. `doc_ids`: non-decreasing along the window; each document has 1 to 8192 tokens and one has exactly 8192.
All inputs are finite; a program needn't handle non-finite values.
Results may differ from the reference program's by a relative error of at most 0.019.
The reference program's roundings to bfloat16 on the way count: a program that leaves them out, or rounds other values in their place, can miss the bound.
Values may be sent and summed in bfloat16 or wider, within the bound.
No kernel may reach another device: no remote copies, remote signals or barrier semaphores. Data moves between devices by JAX's collectives and lax.ppermute only.
A program may use at most 128 MiB of HBM per device.

```python
import math
import jax
import jax.numpy as jnp
import numpy as np
from jax import lax

MODEL_WIDTH = 4096
QUERY_HEADS = 32
KEY_VALUE_HEADS = 8
HEAD_SIZE = 128
WINDOW_TOKENS = 16384
DOC_MOST = 8192
DOC_COUNT = 16


def draw_norm_gain(key, part):
    gains = jax.random.uniform(key, (MODEL_WIDTH,), jnp.float32, 1.2, 2.2)
    return gains.astype(jnp.bfloat16)


def shard_levels(key, shape, split, smallest, high):
    factor_of = 1.0
    for dim, parts in split:
        steps = jax.random.uniform(jax.random.fold_in(jax.random.fold_in(key, 6), dim), (parts,), jnp.float32, smallest / len(split), high / len(split))
        factor_of = factor_of * jnp.repeat(jnp.exp(steps), shape[dim] // parts).reshape((-1,) + (1,) * (len(shape) - 1 - dim))
    return factor_of


def profile(count, total, limit, slope):
    portions = [(1 << 20) // math.isqrt(grade ** slope) + 1 for grade in range(2, count + 1)]
    rest, holding = total - limit - (count - 1), [1] * (count - 1)
    while rest > 0:
        movable = [i for i in range(count - 1) if holding[i] < limit]
        pool, budget = sum([portions[i] for i in movable]), rest
        for i in movable:
            more = min(limit - holding[i], max(1, budget * portions[i] // pool), rest)
            holding[i] = holding[i] + more
            rest = rest - more
    return np.array([limit] + holding)


def ragged_sizes(key, number_of, total, most, slope):
    if number_of == 2:
        one = jax.random.randint(key, (), max(1, total - most), min(most, total - 1) + 1)
        return jnp.stack([one, total - one])
    lengths = jnp.asarray(profile(number_of, total, most, slope), jnp.int32)
    couples = (number_of - 1) // 2
    giver, receiver = lengths[1:1 + 2 * couples:2], lengths[2:2 + 2 * couples:2]
    margin = jnp.minimum(giver - 1, most - receiver)
    passed = jax.random.randint(jax.random.fold_in(key, 1), (couples,), 0, 1 << 20) % (margin + 1)
    lengths = lengths.at[1:1 + 2 * couples:2].set(giver - passed).at[2:2 + 2 * couples:2].set(receiver + passed)
    return lengths[jax.random.permutation(jax.random.fold_in(key, 2), number_of)]


def bell_draw(own_key, dims, width, bound, cuts=(), held_as=jnp.bfloat16):
    loudness = shard_levels(own_key, dims, cuts, -0.22, 0.18) if cuts else 1.0
    drawn = jax.random.normal(own_key, dims, jnp.float32) * width * loudness
    return jnp.minimum(jnp.maximum(drawn, -bound), bound).astype(held_as)


def setup_inputs(seed: int = 0) -> dict:
    streams_of = jax.random.split(jax.random.key(seed), 6)
    return {
        "tokens": bell_draw(streams_of[0], (WINDOW_TOKENS, MODEL_WIDTH), 1.0, 6.0, ((0, 32), (1, 8))),
        "norm_gain": draw_norm_gain(jax.random.fold_in(streams_of[5], 71), 0),
        "query_key_value_weight": bell_draw(streams_of[2], (MODEL_WIDTH, (QUERY_HEADS + 2 * KEY_VALUE_HEADS) * HEAD_SIZE), MODEL_WIDTH ** -0.5, 0.09375, ((1, 8),)),
        "out_weight": bell_draw(streams_of[3], (QUERY_HEADS * HEAD_SIZE, MODEL_WIDTH), (QUERY_HEADS * HEAD_SIZE) ** -0.5, 0.09375, ((0, 8),)),
        "doc_ids": jnp.searchsorted(jnp.cumsum(ragged_sizes(streams_of[4], DOC_COUNT, WINDOW_TOKENS, DOC_MOST, 2)), jnp.arange(WINDOW_TOKENS), side="right").astype(jnp.int32),
    }


epsilon = 1e-05
theta = 500000.0

def rotate(vectors, positions):
    half = vectors.shape[-1] // 2
    inverse = 1.0 / theta ** (jnp.arange(half, dtype=jnp.float32) * (2.0 / vectors.shape[-1]))
    angles = positions.astype(jnp.float32)[:, None] * inverse[None, :]
    cosine = jnp.cos(angles)[:, None, :]
    sine = jnp.sin(angles)[:, None, :]
    first = vectors[..., :half]
    second = vectors[..., half:]
    return jnp.concatenate([first * cosine - second * sine, second * cosine + first * sine], axis=-1)

def reference(tokens, norm_gain, query_key_value_weight, out_weight, doc_ids):
    head_group = QUERY_HEADS // KEY_VALUE_HEADS
    floats = tokens.astype(jnp.float32)
    normed_input = (floats * lax.rsqrt(lax.optimization_barrier(jnp.mean(floats * floats, axis=1, keepdims=True)) + epsilon) * norm_gain.astype(jnp.float32)).astype(jnp.bfloat16)
    mixed_output = jnp.dot(normed_input, query_key_value_weight, preferred_element_type=jnp.float32).reshape(WINDOW_TOKENS, KEY_VALUE_HEADS, (head_group + 2) * HEAD_SIZE)
    positions = jnp.arange(WINDOW_TOKENS, dtype=jnp.int32)
    query_rows = rotate(mixed_output[:, :, :head_group * HEAD_SIZE].reshape(WINDOW_TOKENS, QUERY_HEADS, HEAD_SIZE), positions).astype(jnp.bfloat16)
    keys = rotate(mixed_output[:, :, head_group * HEAD_SIZE:(head_group + 1) * HEAD_SIZE], positions).astype(jnp.bfloat16)
    values = mixed_output[:, :, (head_group + 1) * HEAD_SIZE:].astype(jnp.bfloat16)
    tile_block = 512 if WINDOW_TOKENS % 512 == 0 else WINDOW_TOKENS
    window = min(WINDOW_TOKENS, DOC_MOST + tile_block)
    scale = HEAD_SIZE ** (-0.5)

    def attend(index):
        query_begin = (index * tile_block).astype(jnp.int32)
        key_start = jnp.clip(query_begin + tile_block - window, 0, WINDOW_TOKENS - window).astype(jnp.int32)
        query_portion = lax.dynamic_slice_in_dim(query_rows, query_begin, tile_block, 0).reshape(tile_block, KEY_VALUE_HEADS, head_group, HEAD_SIZE).astype(jnp.float32)
        key_part = lax.dynamic_slice_in_dim(keys, key_start, window, 0).astype(jnp.float32)
        value_part = lax.dynamic_slice_in_dim(values, key_start, window, 0).astype(jnp.float32)
        query_docs = lax.dynamic_slice_in_dim(doc_ids, query_begin, tile_block, 0)
        key_docs = lax.dynamic_slice_in_dim(doc_ids, key_start, window, 0)
        query_positions = query_begin + jnp.arange(tile_block, dtype=jnp.int32)
        key_positions = key_start + jnp.arange(window, dtype=jnp.int32)
        mask = (key_positions[None, :] <= query_positions[:, None]) & (key_docs[None, :] == query_docs[:, None])
        scores = jnp.einsum('qgjd,kgd->gjqk', query_portion, key_part) * scale
        highest = lax.optimization_barrier(jnp.max(jnp.where(mask, scores, -1e+30), axis=-1, keepdims=True))
        weights = jnp.where(mask, jnp.exp(scores - highest), 0.0)
        totals = lax.optimization_barrier(jnp.sum(weights, axis=-1))
        rounded = lax.optimization_barrier(weights.astype(jnp.bfloat16)).astype(jnp.float32)
        summed = jnp.einsum('gjqk,kgd->qgjd', rounded, value_part)
        normal = summed / jnp.transpose(totals, (2, 0, 1))[..., None]
        return normal.astype(jnp.bfloat16).reshape(tile_block, QUERY_HEADS * HEAD_SIZE)
    heads = lax.map(attend, jnp.arange(WINDOW_TOKENS // tile_block, dtype=jnp.int32)).reshape(WINDOW_TOKENS, QUERY_HEADS * HEAD_SIZE)
    return jnp.dot(heads, out_weight, preferred_element_type=jnp.float32).astype(jnp.bfloat16)
```

```python
import jax
import jax.numpy as jnp
from jax import lax
from jax.experimental import pallas as pl
from jax.experimental.pallas import tpu as pltpu
from jax.sharding import PartitionSpec as P

QUERY_HEADS = 32
KEY_VALUE_HEADS = 8
HEAD_SIZE = 128
GROUP = QUERY_HEADS // KEY_VALUE_HEADS
MODEL_WIDTH = 4096

T = 512
HALF = T // 2
PIECE = 512
Y, Z = 4, 8
PIECES = MODEL_WIDTH // PIECE
LANES = 128
KV_ROWS = 2 * T
MSG_ROWS = KV_ROWS + 16

epsilon = 1e-05
theta = 500000.0
floor_score = -1e30
exponent_scale = HEAD_SIZE**-0.5 * 1.4426950408889634

bf16 = jnp.bfloat16
f32 = jnp.float32


def shift(x, axis, distance):
    n = lax.axis_size(axis)
    return lax.ppermute(x, axis, [(i, (i + distance) % n) for i in range(n)])


def shift_z(x):
    return lax.ppermute(
        x, "tok", [(z * Y + y, (z + 1) % Z * Y + y) for z in range(Z) for y in range(Y)]
    )


def shift_y(x, distance):
    return lax.ppermute(
        x, "tok", [(z * Y + y, z * Y + (y + distance) % Y) for z in range(Z) for y in range(Y)]
    )


def vmem(n):
    return [pl.BlockSpec(memory_space=pltpu.VMEM)] * n


def smem():
    return pl.BlockSpec(memory_space=pltpu.SMEM)


def params():
    return pltpu.CompilerParams(vmem_limit_bytes=56 << 20)


def project_kernel(
    fids, x0, p0, m0, q0, r0, x1, p1, m1, q1, r1, weight, cosine, sine, ids,
    queries, message, normed, held, mixed, sem,
):
    fetch = pltpu.make_async_copy(weight, held, sem)
    fetch.start()
    pieces = []
    for x, p, m, q, r in ((x0, p0, m0, q0, r0), (x1, p1, m1, q1, r1)):
        for a in (x, p, m):
            pieces.append(((a, 0), (a, HALF), (a, T)))
        pieces.append(((q, 0), (r, 0), (r, HALF)))
    step_rows = 16
    for half in range(2):

        def step(i, _):
            row = pl.multiple_of(i * step_rows, step_rows)
            total = jnp.zeros((step_rows, PIECE), f32)
            for piece in pieces:
                ref, base = piece[half]
                v = ref[pl.ds(base + row, step_rows), :].astype(f32)
                total += v * v
            mean = jnp.sum(total, axis=1, keepdims=True) * (1.0 / MODEL_WIDTH)
            scale = lax.rsqrt(mean + epsilon)
            for k, piece in enumerate(pieces):
                ref, base = piece[half]
                gain_ref, gain_base = piece[2]
                gain = gain_ref[gain_base : gain_base + 16, :].astype(f32)
                v = ref[pl.ds(base + row, step_rows), :].astype(f32) * scale * gain
                column = pl.multiple_of(fids[k] * PIECE, PIECE)
                normed[pl.ds(half * HALF + row, step_rows), pl.ds(column, PIECE)] = v.astype(bf16)
            return 0

        lax.fori_loop(0, HALF // step_rows, step, 0)
    fetch.wait()

    def columns(i, _):
        at = pl.multiple_of(i * 256, 256)
        mixed[:, pl.ds(at, 256)] = jnp.dot(
            normed[...], held[:, pl.ds(at, 256)], preferred_element_type=f32
        )
        return 0

    lax.fori_loop(0, (GROUP + 2) * HEAD_SIZE // 256, columns, 0)

    def rotated(h):
        v = mixed[:, h * HEAD_SIZE : (h + 1) * HEAD_SIZE]
        return v * cosine[...] + pltpu.roll(v, HEAD_SIZE // 2, 1) * sine[...]

    for h in range(GROUP):
        queries[h * HEAD_SIZE : (h + 1) * HEAD_SIZE, :] = rotated(h).T.astype(bf16)
    message[0:T, :] = rotated(GROUP).astype(bf16)
    for j in range(T // LANES):
        v = mixed[j * LANES : (j + 1) * LANES, (GROUP + 1) * HEAD_SIZE :]
        message[T + j * LANES : T + (j + 1) * LANES, :] = v.T.astype(bf16)
    message[KV_ROWS:MSG_ROWS, :] = ids[...]


def project(fids, pieces, weight, cosine, sine, ids):
    width = (GROUP + 2) * HEAD_SIZE
    return pl.pallas_call(
        project_kernel,
        out_shape=(
            jax.ShapeDtypeStruct((GROUP * HEAD_SIZE, T), bf16),
            jax.ShapeDtypeStruct((MSG_ROWS, LANES), bf16),
        ),
        in_specs=[smem()] + vmem(10) + [pl.BlockSpec(memory_space=pl.ANY)] + vmem(3),
        out_specs=tuple(vmem(2)),
        scratch_shapes=[
            pltpu.VMEM((T, MODEL_WIDTH), bf16),
            pltpu.VMEM((MODEL_WIDTH, width), bf16),
            pltpu.VMEM((T, width), f32),
            pltpu.SemaphoreType.DMA,
        ],
        compiler_params=params(),
        cost_estimate=pl.CostEstimate(
            flops=2 * T * MODEL_WIDTH * width, transcendentals=0, bytes_accessed=12 << 20
        ),
        name="project",
    )(fids, *pieces, weight, cosine, sine, ids)


def attend_block(block, queries, highest, totals, accum, mask):
    keys = block[0:T, :]
    values = jnp.concatenate(
        [block[T + j * LANES : T + (j + 1) * LANES, :] for j in range(T // LANES)], axis=1
    )

    def head(h, _):
        rows = pl.ds(pl.multiple_of(h * HEAD_SIZE, HEAD_SIZE), HEAD_SIZE)
        for at in range(0, T, LANES):
            part = slice(at, at + LANES)
            scores = jnp.dot(keys, queries[rows, part], preferred_element_type=f32)
            if mask is not None:
                scores = mask(scores, at)
            old = highest[h, :, part]
            new = jnp.maximum(old, jnp.max(scores, axis=0, keepdims=True))
            weights = jnp.exp2((scores - new) * exponent_scale)
            fade = jnp.exp2((old - new) * exponent_scale)
            highest[h, :, part] = new
            totals[h, :, part] = totals[h, :, part] * fade + jnp.sum(weights, axis=0, keepdims=True)
            accum[rows, part] = accum[rows, part] * fade + jnp.dot(
                values, weights.astype(bf16), preferred_element_type=f32
            )
        return 0

    lax.fori_loop(0, GROUP, head, 0)


def attend_own(block, queries, doc_rows, doc_columns, highest, totals, accum):
    highest[...] = jnp.full(highest.shape, floor_score, f32)
    totals[...] = jnp.zeros(totals.shape, f32)
    accum[...] = jnp.zeros(accum.shape, f32)

    def mask(scores, at):
        key = lax.broadcasted_iota(jnp.int32, scores.shape, 0)
        query = lax.broadcasted_iota(jnp.int32, scores.shape, 1) + at
        same = doc_rows[...] == doc_columns[0:1, at : at + LANES]
        return jnp.where((key <= query) & same, scores, floor_score)

    attend_block(block, queries, highest, totals, accum, mask)


def attend_earlier(info, which, copies, queries, block, highest, totals, accum):
    own, first_doc, span = info[0], info[1], info[2]

    def step(k, _):
        index = info[3 + which[0]]
        for j in range(1, len(which)):
            index = jnp.where(k == j, info[3 + which[j]], index)

        @pl.when((index >= 0) & (index < own))
        def _():
            for j, copy in enumerate(copies):
                pl.when(k == j)(copy)
            ids = block[KV_ROWS:MSG_ROWS, :].astype(f32)
            low = jnp.sum(jnp.where(ids < first_doc.astype(f32), 1.0, 0.0)).astype(jnp.int32)

            @pl.when((low == 0) & (span == T))
            def _():
                attend_block(block, queries, highest, totals, accum, None)

            @pl.when((low < T) & ((low > 0) | (span < T)))
            def _():
                def mask(scores, at):
                    key = lax.broadcasted_iota(jnp.int32, scores.shape, 0)
                    query = lax.broadcasted_iota(jnp.int32, scores.shape, 1) + at
                    return jnp.where((key >= low) & (query < span), scores, floor_score)

                attend_block(block, queries, highest, totals, accum, mask)

        return 0

    lax.fori_loop(0, len(which), step, 0)


STATE = (
    jax.ShapeDtypeStruct((GROUP, 1, T), f32),
    jax.ShapeDtypeStruct((GROUP, 1, T), f32),
    jax.ShapeDtypeStruct((GROUP * HEAD_SIZE, T), f32),
)
BLOCK_FLOPS = 4 * GROUP * T * T * HEAD_SIZE


def attend_first(queries, message, doc_rows, doc_columns):
    def kernel(message, queries, doc_rows, doc_columns, highest, totals, accum):
        attend_own(message, queries, doc_rows, doc_columns, highest, totals, accum)

    return pl.pallas_call(
        kernel,
        out_shape=STATE,
        in_specs=vmem(4),
        out_specs=tuple(vmem(3)),
        compiler_params=params(),
        cost_estimate=pl.CostEstimate(
            flops=2 * BLOCK_FLOPS, transcendentals=GROUP * T * T, bytes_accessed=2 << 20
        ),
        name="attend_own",
    )(message, queries, doc_rows, doc_columns)


def pair_of(keys, base, values):
    def copy_into(block):
        block[0:T, :] = keys[base : base + T, :]
        block[T:MSG_ROWS, :] = values[base : base + MSG_ROWS - T, :]

    return copy_into


def whole_of(ref):
    def copy_into(block):
        block[...] = ref[0:MSG_ROWS, :]

    return copy_into


def attend_stage(info, queries, state, along, against, straight, between, which):
    n = 2 + (straight is not None)

    def kernel(info, queries, *refs):
        blocks = refs[:n]
        old, new, block = refs[n : n + 3], refs[n + 3 : n + 6], refs[n + 6]
        for a, b in zip(old, new):
            b[...] = a[...]
        makers = [whole_of(b) for b in blocks]
        if between:
            makers.append(pair_of(blocks[0], MSG_ROWS, blocks[1]))
        copies = [lambda make=make: make(block) for make in makers]
        attend_earlier(info, which, copies, queries, block, *new)

    blocks = [along, against] + ([straight] if straight is not None else [])
    return pl.pallas_call(
        kernel,
        out_shape=STATE,
        in_specs=[smem()] + vmem(1 + n + 3),
        out_specs=tuple(vmem(3)),
        scratch_shapes=[pltpu.VMEM((MSG_ROWS, LANES), bf16)],
        input_output_aliases={2 + n + i: i for i in range(3)},
        compiler_params=params(),
        cost_estimate=pl.CostEstimate(
            flops=2 * len(which) * BLOCK_FLOPS,
            transcendentals=len(which) * GROUP * T * T,
            bytes_accessed=3 << 20,
        ),
        name="attend_stage",
    )(info, queries, *blocks, *state)


def fetch_columns(columns, weight, held, sems, count):
    fetches = []
    for k in range(count):
        at = pl.multiple_of(columns[k] * PIECE, PIECE)
        fetches.append(pltpu.make_async_copy(weight.at[:, pl.ds(at, PIECE)], held.at[k], sems.at[k]))
    for fetch in fetches:
        fetch.start()
    return fetches


def finish(info, queries, state, keys, values, which, columns, weight):
    def kernel(
        info, columns, queries, keys, values, old_highest, old_totals, old_accum, weight,
        heads, first, others, highest, totals, accum, block, held, sems,
    ):
        fetches = fetch_columns(columns, weight, held, sems, 4)
        highest[...] = old_highest[...]
        totals[...] = old_totals[...]
        accum[...] = old_accum[...]
        make = pair_of(keys, 0, values)
        attend_earlier(
            info, which, [lambda: make(block)], queries, block, highest, totals, accum
        )
        for h in range(GROUP):
            rows = slice(h * HEAD_SIZE, (h + 1) * HEAD_SIZE)
            heads[:, rows] = (accum[rows, :] / totals[h]).T.astype(bf16)
        for k in range(4):
            fetches[k].wait()
            made = jnp.dot(heads[...], held[k], preferred_element_type=f32).astype(bf16)
            if k == 0:
                first[...] = made
            else:
                others[k - 1] = made

    return pl.pallas_call(
        kernel,
        out_shape=(
            jax.ShapeDtypeStruct((T, GROUP * HEAD_SIZE), bf16),
            jax.ShapeDtypeStruct((T, PIECE), bf16),
            jax.ShapeDtypeStruct((3, T, PIECE), bf16),
        ),
        in_specs=[smem(), smem()] + vmem(6) + [pl.BlockSpec(memory_space=pl.ANY)],
        out_specs=tuple(vmem(3)),
        scratch_shapes=[
            pltpu.VMEM((GROUP, 1, T), f32),
            pltpu.VMEM((GROUP, 1, T), f32),
            pltpu.VMEM((GROUP * HEAD_SIZE, T), f32),
            pltpu.VMEM((MSG_ROWS, LANES), bf16),
            pltpu.VMEM((4, GROUP * HEAD_SIZE, PIECE), bf16),
            pltpu.SemaphoreType.DMA((4,)),
        ],
        compiler_params=params(),
        cost_estimate=pl.CostEstimate(
            flops=2 * T * T * MODEL_WIDTH, transcendentals=0, bytes_accessed=8 << 20
        ),
        name="finish",
    )(info, columns, queries, keys, values, *state, weight)


def own_products(columns, heads, weight):
    def kernel(columns, heads, weight, out, held, sems):
        fetches = fetch_columns(columns, weight, held, sems, 4)
        for k in range(4):
            fetches[k].wait()
            out[k] = jnp.dot(heads[...], held[k], preferred_element_type=f32)

    return pl.pallas_call(
        kernel,
        out_shape=jax.ShapeDtypeStruct((4, T, PIECE), f32),
        in_specs=[smem()] + vmem(1) + [pl.BlockSpec(memory_space=pl.ANY)],
        out_specs=vmem(1)[0],
        scratch_shapes=[
            pltpu.VMEM((4, GROUP * HEAD_SIZE, PIECE), bf16),
            pltpu.SemaphoreType.DMA((4,)),
        ],
        compiler_params=params(),
        cost_estimate=pl.CostEstimate(
            flops=2 * T * T * MODEL_WIDTH // 2, transcendentals=0, bytes_accessed=6 << 20
        ),
        name="own_products",
    )(columns, heads, weight)


def body(tokens, norm_gain, query_key_value_weight, out_weight, doc_ids):
    shard = lax.axis_index("tok")
    chip = lax.axis_index("head")
    core = lax.axis_index("grp")
    row, column = shard // Y, shard % Y

    own = jnp.concatenate([tokens, jnp.broadcast_to(norm_gain[None, :], (16, PIECE))], axis=0)
    behind = shift(own, "head", 1)
    ahead = shift(own, "head", -1)
    across = shift(own, "grp", 1)
    top = shift(behind[:HALF], "head", 1)
    bottom = shift(ahead[HALF:], "head", -1)
    mine = [own, behind, ahead, top, bottom]
    theirs = [across] + [shift(a, "grp", 1) for a in mine[1:]]
    chips = jnp.stack([chip, (chip - 1) % 4, (chip + 1) % 4, (chip + 2) % 4])
    fids = jnp.concatenate([chips * 2 + core, chips * 2 + 1 - core]).astype(jnp.int32)

    positions = shard * T + jnp.arange(T, dtype=jnp.int32)
    half = HEAD_SIZE // 2
    inverse = 1.0 / theta ** (jnp.arange(half, dtype=f32) * (2.0 / HEAD_SIZE))
    angles = positions.astype(f32)[:, None] * inverse[None, :]
    cosine, sine = jnp.cos(angles), jnp.sin(angles)
    cosine = jnp.concatenate([cosine, cosine], axis=1)
    sine = jnp.concatenate([-sine, sine], axis=1)
    ids = jnp.concatenate(
        [doc_ids.reshape(T // LANES, LANES), jnp.full((16 - T // LANES, LANES), 99, jnp.int32)]
    ).astype(bf16)
    doc_rows = jnp.broadcast_to(doc_ids.astype(f32)[:, None], (T, LANES))
    doc_columns = jnp.broadcast_to(doc_ids.astype(f32)[None, :], (8, T))

    queries, message = project(fids, mine + theirs, query_key_value_weight, cosine, sine, ids)

    blocks = [4 * (row - s) + (column + k) % Y for s in range(5) for k in range(4)]
    info = jnp.stack(
        [shard, doc_ids[0], jnp.sum((doc_ids == doc_ids[0]).astype(jnp.int32))] + blocks
    ).astype(jnp.int32)

    straight = message
    state = attend_first(queries, message, doc_rows, doc_columns)
    along, against = message, message
    for s in range(5):
        next_along = shift_y(along, 1)
        next_against = shift_y(against, -1)
        following = shift_z(straight) if s < 4 else None
        which = [4 * s + 3, 4 * s + 1]
        if s < 4:
            which.append(4 * (s + 1))
        if s > 0:
            which.append(4 * (s - 1) + 2)
        state = attend_stage(
            info, queries, state, next_along, next_against, following, s > 0, which
        )
        forward, backward = next_along[0:T], next_against[T:MSG_ROWS]
        if s < 4:
            straight = following
            along = jnp.concatenate([straight, forward], axis=0)
            against = jnp.concatenate([straight, backward], axis=0)
    keys = shift_y(forward, 1)
    values = shift_y(backward, -1)

    order = jnp.stack([(chip + 2) % 4, (chip + 1) % 4, (chip + 3) % 4, chip])
    heads, first, others = finish(
        info, queries, state, keys, values, [4 * 4 + 2],
        (order * 2 + 1 - core).astype(jnp.int32), out_weight,
    )
    first = shift(first, "grp", 1)
    others = shift(others, "grp", 1)
    products = own_products((order * 2 + core).astype(jnp.int32), heads, out_weight)

    far = (products[0] + first.astype(f32)).astype(bf16)
    far_up = shift(far[:HALF], "head", 1)
    far_down = shift(far[HALF:], "head", -1)
    up_low = shift((products[1, HALF:] + others[0, HALF:].astype(f32)).astype(bf16), "head", 1)
    down_high = shift((products[2, :HALF] + others[1, :HALF].astype(f32)).astype(bf16), "head", -1)
    up_high = products[1, :HALF] + others[0, :HALF].astype(f32) + far_up.astype(f32)
    down_low = products[2, HALF:] + others[1, HALF:].astype(f32) + far_down.astype(f32)
    up_high = shift(up_high.astype(bf16), "head", 1)
    down_low = shift(down_low.astype(bf16), "head", -1)
    kept = products[3] + others[2].astype(f32)
    return jnp.concatenate(
        [
            kept[:HALF] + up_high.astype(f32) + down_high.astype(f32),
            kept[HALF:] + up_low.astype(f32) + down_low.astype(f32),
        ]
    ).astype(bf16)


def solution(mesh):
    return jax.shard_map(
        body,
        mesh=mesh,
        in_specs=(
            P("tok", ("head", "grp")),
            P(("head", "grp")),
            P(None, ("head", "grp")),
            P(("head", "grp"), None),
            P("tok"),
        ),
        out_specs=P("tok", ("head", "grp")),
        check_vma=False,
    )
```

```python
import jax
import jax.numpy as jnp
from jax import lax
from jax.experimental import pallas as pl
from jax.experimental.pallas import tpu as pltpu
from jax.sharding import PartitionSpec as P


QUERY_HEADS = 32
KEY_VALUE_HEADS = 8
HEAD_SIZE = 128
GROUP = QUERY_HEADS // KEY_VALUE_HEADS
MODEL_WIDTH = 4096

T = 512
HALF = T // 2
PIECE = 512
Y, Z = 4, 8
LANES = 128
KV_ROWS = 2 * T
MSG_ROWS = KV_ROWS + 16

epsilon = 1e-05
theta = 500000.0
floor_score = -1e30
exponent_scale = HEAD_SIZE**-0.5 * 1.4426950408889634

bf16 = jnp.bfloat16
f32 = jnp.float32


def shift(x, axis, distance):
    n = lax.axis_size(axis)
    return lax.ppermute(x, axis, [(i, (i + distance) % n) for i in range(n)])


def shift_z(x):
    return lax.ppermute(
        x, "tok", [(z * Y + y, (z + 1) % Z * Y + y) for z in range(Z) for y in range(Y)]
    )


def shift_y(x, distance):
    return lax.ppermute(
        x, "tok", [(z * Y + y, z * Y + (y + distance) % Y) for z in range(Z) for y in range(Y)]
    )


def vmem(n):
    return [pl.BlockSpec(memory_space=pltpu.VMEM)] * n


def smem():
    return pl.BlockSpec(memory_space=pltpu.SMEM)


def params():
    return pltpu.CompilerParams(vmem_limit_bytes=56 << 20)


def project_kernel(
    fids, x0, p0, m0, q0, r0, x1, pm1, qr1, weight, cosine, sine, ids,
    queries, message, normed, held, mixed, sems,
):
    fetches = []
    for i in range(3):
        part = slice(i * 256, (i + 1) * 256)
        fetches.append(pltpu.make_async_copy(weight.at[:, part], held.at[i], sems.at[i]))
    for fetch in fetches:
        fetch.start()
    pieces = []
    rows = T + 16
    mine = ((x0, 0), (p0, 0), (m0, 0), (q0, 0), (r0, 0))
    theirs = ((x1, 0), (pm1, 0), (pm1, rows), (qr1, 0), (qr1, HALF))
    for *three, (q, top), (r, bottom) in (mine, theirs):
        for ref, base in three:
            pieces.append(((ref, base), (ref, base + HALF), (ref, base + T)))
        pieces.append(((q, top), (r, bottom), (r, bottom + HALF)))
    step_rows = 16
    for half in range(2):

        def step(i, _):
            row = pl.multiple_of(i * step_rows, step_rows)
            total = jnp.zeros((step_rows, PIECE), f32)
            for piece in pieces:
                ref, base = piece[half]
                v = ref[pl.ds(base + row, step_rows), :].astype(f32)
                total += v * v
            mean = jnp.sum(total, axis=1, keepdims=True) * (1.0 / MODEL_WIDTH)
            scale = lax.rsqrt(mean + epsilon)
            for k, piece in enumerate(pieces):
                ref, base = piece[half]
                gain_ref, gain_base = piece[2]
                gain = gain_ref[gain_base : gain_base + 16, :].astype(f32)
                v = ref[pl.ds(base + row, step_rows), :].astype(f32) * scale * gain
                column = pl.multiple_of(fids[k] * PIECE, PIECE)
                normed[pl.ds(half * HALF + row, step_rows), pl.ds(column, PIECE)] = v.astype(bf16)
            return 0

        lax.fori_loop(0, HALF // step_rows, step, 0)

    def columns(i, _):
        for j in range(3):
            pl.when(i == j)(fetches[j].wait)
        at = pl.multiple_of(i * 256, 256)
        mixed[:, pl.ds(at, 256)] = jnp.dot(normed[...], held[i], preferred_element_type=f32)
        return 0

    lax.fori_loop(0, (GROUP + 2) * HEAD_SIZE // 256, columns, 0)

    def rotated(h):
        v = mixed[:, h * HEAD_SIZE : (h + 1) * HEAD_SIZE]
        return v * cosine[...] + pltpu.roll(v, HEAD_SIZE // 2, 1) * sine[...]

    for h in range(GROUP):
        queries[h * HEAD_SIZE : (h + 1) * HEAD_SIZE, :] = rotated(h).astype(bf16).T
    message[0:T, :] = rotated(GROUP).astype(bf16)
    for j in range(T // LANES):
        v = mixed[j * LANES : (j + 1) * LANES, (GROUP + 1) * HEAD_SIZE :]
        message[T + j * LANES : T + (j + 1) * LANES, :] = v.astype(bf16).T
    message[KV_ROWS:MSG_ROWS, :] = ids[...]


def project(fids, pieces, weight, cosine, sine, ids):
    width = (GROUP + 2) * HEAD_SIZE
    return pl.pallas_call(
        project_kernel,
        out_shape=(
            jax.ShapeDtypeStruct((GROUP * HEAD_SIZE, T), bf16),
            jax.ShapeDtypeStruct((MSG_ROWS, LANES), bf16),
        ),
        in_specs=[smem()] + vmem(8) + [pl.BlockSpec(memory_space=pl.ANY)] + vmem(3),
        out_specs=tuple(vmem(2)),
        scratch_shapes=[
            pltpu.VMEM((T, MODEL_WIDTH), bf16),
            pltpu.VMEM((3, MODEL_WIDTH, 256), bf16),
            pltpu.VMEM((T, width), f32),
            pltpu.SemaphoreType.DMA((3,)),
        ],
        compiler_params=params(),
        cost_estimate=pl.CostEstimate(
            flops=2 * T * MODEL_WIDTH * width, transcendentals=0, bytes_accessed=12 << 20
        ),
        name="project",
    )(fids, *pieces, weight, cosine, sine, ids)


def attend_block(block, queries, highest, totals, accum, change, together):
    keys = block[0:T, :]
    values = jnp.concatenate(
        [block[T + j * LANES : T + (j + 1) * LANES, :] for j in range(T // LANES)], axis=1
    )

    def head(h):
        rows = pl.ds(pl.multiple_of(h * HEAD_SIZE, HEAD_SIZE), HEAD_SIZE)
        for at in range(0, T, LANES):
            part = slice(at, at + LANES)
            scores = jnp.dot(keys, queries[rows, part], preferred_element_type=f32)
            scores = change(scores, at)
            old = highest[h, :, part]
            new = jnp.maximum(old, jnp.max(scores, axis=0, keepdims=True))
            weights = jnp.exp2((scores - new) * exponent_scale)
            fade = jnp.exp2((old - new) * exponent_scale)
            highest[h, :, part] = new
            totals[h, :, part] = totals[h, :, part] * fade + jnp.sum(weights, axis=0, keepdims=True)
            accum[rows, part] = accum[rows, part] * fade + jnp.dot(
                values, weights.astype(bf16), preferred_element_type=f32
            )

    def heads(i, _):
        for j in range(together):
            head(i * together + j)
        return 0

    lax.fori_loop(0, GROUP // together, heads, 0)


def clear(highest, totals, accum):
    highest[...] = jnp.full(highest.shape, floor_score, f32)
    totals[...] = jnp.zeros(totals.shape, f32)
    accum[...] = jnp.zeros(accum.shape, f32)


def whole_of(ref):
    def copies(block, sems):
        return [pltpu.make_async_copy(ref.at[pl.ds(0, MSG_ROWS)], block, sems.at[0])]

    return copies


def pair_of(keys, base, values, value_base):
    rest = MSG_ROWS - T

    def copies(block, sems):
        return [
            pltpu.make_async_copy(keys.at[pl.ds(base, T)], block.at[pl.ds(0, T)], sems.at[0]),
            pltpu.make_async_copy(
                values.at[pl.ds(value_base, rest)], block.at[pl.ds(T, rest)], sems.at[1]
            ),
        ]

    return copies


def attend_earlier(info, which, sources, queries, blocks, bias, sems, fill, state):
    own, first_doc = info[0], info[1].astype(f32)

    def reached(j):
        index = info[3 + which[j]]
        return (index >= 0) & (index < own)

    def each(j, act):
        def run():
            for copy in sources[j](blocks.at[j], sems.at[j]):
                act(copy)

        return run

    for j in range(len(which)):
        pl.when(reached(j))(each(j, lambda copy: copy.start()))
    fill()

    def step(k, _):
        wanted = reached(0)
        for j in range(1, len(which)):
            wanted = jnp.where(k == j, reached(j), wanted)

        @pl.when(wanted)
        def _():
            for j in range(len(which)):
                pl.when(k == j)(each(j, lambda copy: copy.wait()))
            block = blocks.at[k]
            ids = block[KV_ROWS:MSG_ROWS, :].astype(f32)
            low = jnp.sum(jnp.where(ids < first_doc, 1.0, 0.0)).astype(jnp.int32)

            @pl.when(low < T)
            def _():
                key = lax.broadcasted_iota(jnp.int32, (T, LANES), 0)
                bias[...] = jnp.where(key < low, floor_score, 0.0)
                attend_block(block, queries, *state, lambda scores, at: scores + bias[...], 1 if len(which) == 3 and which[0] == 3 else TOGETHER)

        return 0

    lax.fori_loop(0, len(which), step, 0)


TOGETHER = 2
STATE = (
    jax.ShapeDtypeStruct((GROUP, 1, T), f32),
    jax.ShapeDtypeStruct((GROUP, 1, T), f32),
    jax.ShapeDtypeStruct((GROUP * HEAD_SIZE, T), f32),
)
BLOCK_FLOPS = 4 * GROUP * T * T * HEAD_SIZE


def earlier_scratch(n):
    return [
        pltpu.VMEM((n, MSG_ROWS, LANES), bf16),
        pltpu.VMEM((T, LANES), f32),
        pltpu.SemaphoreType.DMA((n, 2)),
    ]


def attend_first(queries, message, doc_rows, doc_columns):
    def kernel(message, queries, doc_rows, doc_columns, *state):
        clear(*state)

        def change(scores, at):
            key = lax.broadcasted_iota(jnp.int32, scores.shape, 0)
            query = lax.broadcasted_iota(jnp.int32, scores.shape, 1) + at
            same = doc_rows[...] == doc_columns[0:1, at : at + LANES]
            return jnp.where((key <= query) & same, scores, floor_score)

        attend_block(message, queries, *state, change, 1)

    return pl.pallas_call(
        kernel,
        out_shape=STATE,
        in_specs=vmem(4),
        out_specs=tuple(vmem(3)),
        compiler_params=params(),
        cost_estimate=pl.CostEstimate(
            flops=2 * BLOCK_FLOPS, transcendentals=GROUP * T * T, bytes_accessed=2 << 20
        ),
        name="attend_own",
    )(message, queries, doc_rows, doc_columns)


def attend_stage(info, queries, state, along, against, straight, between, which):
    n = 2 + (straight is not None)

    def kernel(info, queries, *refs):
        refs = list(refs)
        messages = [refs.pop(0) for _ in range(n)]
        old = [refs.pop(0) for _ in state]
        new = [refs.pop(0) for _ in range(3)]

        def fill():
            if old:
                for a, b in zip(old, new):
                    b[...] = a[...]
            else:
                clear(*new)

        sources = [whole_of(m) for m in messages]
        if between:
            sources.append(pair_of(messages[0], MSG_ROWS, messages[1], MSG_ROWS))
        attend_earlier(info, which, sources, queries, *refs, fill, new)

    messages = [along, against] + ([straight] if straight is not None else [])
    return pl.pallas_call(
        kernel,
        out_shape=STATE,
        in_specs=[smem()] + vmem(1) + [pl.BlockSpec(memory_space=pl.ANY)] * n + vmem(len(state)),
        out_specs=tuple(vmem(3)),
        scratch_shapes=earlier_scratch(len(which)),
        input_output_aliases={2 + n + i: i for i in range(len(state))},
        compiler_params=params(),
        cost_estimate=pl.CostEstimate(
            flops=2 * len(which) * BLOCK_FLOPS,
            transcendentals=len(which) * GROUP * T * T,
            bytes_accessed=3 << 20,
        ),
        name="attend_stage",
    )(info, queries, *messages, *state)


def fetch_columns(columns, first, count, weight, held, sems):
    fetches = []
    for k in range(count):
        at = pl.multiple_of(columns[first + k] * PIECE, PIECE)
        fetches.append(pltpu.make_async_copy(weight.at[:, pl.ds(at, PIECE)], held.at[k], sems.at[k]))
    for fetch in fetches:
        fetch.start()
    return fetches


def column_scratch(count):
    return [
        pltpu.VMEM((count, GROUP * HEAD_SIZE, PIECE), bf16),
        pltpu.SemaphoreType.DMA((count,)),
    ]


def finish(info, queries, own_state, state, keys, values, which, columns, weight):
    def kernel(
        info, columns, queries, keys, values, own_highest, own_totals, own_accum,
        old_highest, old_totals, old_accum, weight,
        heads, first, others, far, highest, totals, accum, blocks, bias, sems, held, held_sems,
    ):
        fetches = fetch_columns(columns, 0, 5, weight, held, held_sems)

        def fill():
            highest[...] = old_highest[...]
            totals[...] = old_totals[...]
            accum[...] = old_accum[...]

        attend_earlier(
            info, which, [pair_of(keys, 0, values, 0)], queries, blocks, bias, sems, fill,
            (highest, totals, accum),
        )
        query = lax.broadcasted_iota(jnp.int32, (1, T), 1)
        for h in range(GROUP):
            rows = slice(h * HEAD_SIZE, (h + 1) * HEAD_SIZE)
            used = (query < info[2]) & (totals[h] > 0.0)
            near, past = own_highest[h], highest[h]
            top = jnp.where(used, jnp.maximum(near, past), near)
            near = jnp.exp2((near - top) * exponent_scale)
            past = jnp.where(used, jnp.exp2((past - top) * exponent_scale), 0.0)
            total = own_totals[h] * near + totals[h] * past
            summed = own_accum[rows, :] * near + accum[rows, :] * past
            heads[:, rows] = (summed / total).astype(bf16).T

        def multiply(k, _):
            for j in range(5):
                pl.when(k == j)(fetches[j].wait)
            far[...] = jnp.dot(heads[...], held[k], preferred_element_type=f32)

            @pl.when(k == 0)
            def _():
                first[...] = far[...].astype(bf16)

            @pl.when((k > 0) & (k < 4))
            def _():
                others[jnp.clip(k - 1, 0, 2)] = far[...].astype(bf16)

            return 0

        lax.fori_loop(0, 5, multiply, 0)

    return pl.pallas_call(
        kernel,
        out_shape=(
            jax.ShapeDtypeStruct((T, GROUP * HEAD_SIZE), bf16),
            jax.ShapeDtypeStruct((T, PIECE), bf16),
            jax.ShapeDtypeStruct((3, T, PIECE), bf16),
            jax.ShapeDtypeStruct((T, PIECE), f32),
        ),
        in_specs=[smem(), smem()]
        + vmem(1)
        + [pl.BlockSpec(memory_space=pl.ANY)] * 2
        + vmem(6)
        + [pl.BlockSpec(memory_space=pl.ANY)],
        out_specs=tuple(vmem(4)),
        scratch_shapes=[
            pltpu.VMEM((GROUP, 1, T), f32),
            pltpu.VMEM((GROUP, 1, T), f32),
            pltpu.VMEM((GROUP * HEAD_SIZE, T), f32),
        ]
        + earlier_scratch(1)
        + column_scratch(5),
        compiler_params=params(),
        cost_estimate=pl.CostEstimate(
            flops=2 * T * T * MODEL_WIDTH, transcendentals=0, bytes_accessed=8 << 20
        ),
        name="finish",
    )(info, columns, queries, keys, values, *own_state, *state, weight)


def own_products(columns, heads, weight):
    def kernel(columns, heads, weight, out, held, sems):
        fetches = fetch_columns(columns, 5, 3, weight, held, sems)

        def multiply(k, _):
            for j in range(3):
                pl.when(k == j)(fetches[j].wait)
            out[k] = jnp.dot(heads[...], held[k], preferred_element_type=f32)
            return 0

        lax.fori_loop(0, 3, multiply, 0)

    return pl.pallas_call(
        kernel,
        out_shape=jax.ShapeDtypeStruct((3, T, PIECE), f32),
        in_specs=[smem()] + vmem(1) + [pl.BlockSpec(memory_space=pl.ANY)],
        out_specs=vmem(1)[0],
        scratch_shapes=column_scratch(3),
        compiler_params=params(),
        cost_estimate=pl.CostEstimate(
            flops=2 * T * T * MODEL_WIDTH // 2, transcendentals=0, bytes_accessed=6 << 20
        ),
        name="own_products",
    )(columns, heads, weight)


def body(tokens, norm_gain, query_key_value_weight, out_weight, doc_ids):
    shard = lax.axis_index("tok")
    chip = lax.axis_index("head")
    core = lax.axis_index("grp")
    row, column = shard // Y, shard % Y

    own = jnp.concatenate([tokens, jnp.broadcast_to(norm_gain[None, :], (16, PIECE))], axis=0)
    behind = shift(own, "head", 1)
    ahead = shift(own, "head", -1)
    across = shift(own, "grp", 1)
    chips = jnp.stack([chip, (chip - 1) % 4, (chip + 1) % 4, (chip + 2) % 4])
    fids = jnp.concatenate([chips * 2 + core, chips * 2 + 1 - core]).astype(jnp.int32)

    positions = shard * T + jnp.arange(T, dtype=jnp.int32)
    half = HEAD_SIZE // 2
    inverse = 1.0 / theta ** (jnp.arange(half, dtype=f32) * (2.0 / HEAD_SIZE))
    angles = positions.astype(f32)[:, None] * inverse[None, :]
    cosine, sine = jnp.cos(angles), jnp.sin(angles)
    cosine = jnp.concatenate([cosine, cosine], axis=1)
    sine = jnp.concatenate([-sine, sine], axis=1)
    ids = jnp.concatenate(
        [doc_ids.reshape(T // LANES, LANES), jnp.full((16 - T // LANES, LANES), 99, jnp.int32)]
    ).astype(bf16)
    doc_rows = jnp.broadcast_to(doc_ids.astype(f32)[:, None], (T, LANES))
    doc_columns = jnp.broadcast_to(doc_ids.astype(f32)[None, :], (8, T))

    blocks = [4 * (row - s) + (column + k) % Y for s in range(5) for k in range(4)]
    info = jnp.stack(
        [shard, doc_ids[0], jnp.sum((doc_ids == doc_ids[0]).astype(jnp.int32))] + blocks
    ).astype(jnp.int32)
    order = jnp.stack([(chip + 2) % 4, (chip + 1) % 4, (chip + 3) % 4, chip])
    columns = jnp.concatenate([order * 2 + 1 - core, order * 2 + core]).astype(jnp.int32)

    behind, ahead, across = lax.optimization_barrier((behind, ahead, across))
    top = shift(behind[:HALF], "head", 1)
    bottom = shift(ahead[HALF:], "head", -1)
    across_near = shift(jnp.concatenate([behind, ahead]), "grp", 1)
    top, bottom, fids, info, columns, cosine, sine, ids, doc_rows, doc_columns = (
        lax.optimization_barrier(
            (top, bottom, fids, info, columns, cosine, sine, ids, doc_rows, doc_columns)
        )
    )
    mine = [own, behind, ahead, top, bottom]
    across_far = shift(jnp.concatenate([top, bottom]), "grp", 1)
    theirs = [across, across_near, across_far]
    queries, message = project(fids, mine + theirs, query_key_value_weight, cosine, sine, ids)

    straight = message
    own_state = attend_first(queries, message, doc_rows, doc_columns)
    state = ()
    along, against = message, message
    for s in range(5):
        next_along = shift_y(along, 1)
        next_against = shift_y(against, -1)
        following = shift_z(straight) if s < 4 else None
        which = [4 * s + 3, 4 * s + 1]
        if s < 4:
            which.append(4 * (s + 1))
        if s > 0:
            which.append(4 * (s - 1) + 2)
        state = attend_stage(
            info, queries, state, next_along, next_against, following, s > 0, which
        )
        forward, backward = next_along[0:T], next_against[T:MSG_ROWS]
        if s < 4:
            straight = following
            along = jnp.concatenate([straight, forward], axis=0)
            against = jnp.concatenate([straight, backward], axis=0)
    keys = shift_y(forward, 1)
    values = shift_y(backward, -1)

    heads, first, others, products = finish(
        info, queries, own_state, state, keys, values, [4 * 4 + 2], columns, out_weight
    )
    first = shift(first, "grp", 1)
    others = shift(others, "grp", 1)
    own_three = own_products(columns, heads, out_weight)

    far = (products + first.astype(f32)).astype(bf16)
    far_up = shift(far[:HALF], "head", 1)
    far_down = shift(far[HALF:], "head", -1)
    products = own_three
    up_low = (products[0, HALF:] + others[0, HALF:].astype(f32)).astype(bf16)
    down_high = (products[1, :HALF] + others[1, :HALF].astype(f32)).astype(bf16)
    up_low = shift(up_low, "head", 1)
    down_high = shift(down_high, "head", -1)
    up_high = products[0, :HALF] + others[0, :HALF].astype(f32) + far_up.astype(f32)
    down_low = products[1, HALF:] + others[1, HALF:].astype(f32) + far_down.astype(f32)
    up_high = shift(up_high.astype(bf16), "head", 1)
    down_low = shift(down_low.astype(bf16), "head", -1)
    kept = products[2] + others[2].astype(f32)
    return jnp.concatenate(
        [
            kept[:HALF] + up_high.astype(f32) + down_high.astype(f32),
            kept[HALF:] + up_low.astype(f32) + down_low.astype(f32),
        ]
    ).astype(bf16)


def solution(mesh):
    return jax.shard_map(
        body,
        mesh=mesh,
        in_specs=(
            P("tok", ("head", "grp")),
            P(("head", "grp")),
            P(None, ("head", "grp")),
            P(("head", "grp"), None),
            P("tok"),
        ),
        out_specs=P("tok", ("head", "grp")),
        check_vma=False,
    )
```

```python
import jax
import jax.numpy as jnp
from jax import lax
from jax.experimental import pallas as pl
from jax.experimental.pallas import tpu as pltpu
from jax.sharding import PartitionSpec as P


QUERY_HEADS = 32
KEY_VALUE_HEADS = 8
HEAD_SIZE = 128
GROUP = QUERY_HEADS // KEY_VALUE_HEADS
MODEL_WIDTH = 4096

T = 512
HALF = T // 2
PIECE = 512
Y, Z = 4, 8
LANES = 128
KV_ROWS = 2 * T
MSG_ROWS = KV_ROWS + 16

epsilon = 1e-05
theta = 500000.0
floor_score = -1e30
exponent_scale = HEAD_SIZE**-0.5 * 1.4426950408889634

bf16 = jnp.bfloat16
f32 = jnp.float32


def shift(x, axis, distance):
    n = lax.axis_size(axis)
    return lax.ppermute(x, axis, [(i, (i + distance) % n) for i in range(n)])


def shift_z(x):
    return lax.ppermute(
        x, "tok", [(z * Y + y, (z + 1) % Z * Y + y) for z in range(Z) for y in range(Y)]
    )


def shift_y(x, distance):
    return lax.ppermute(
        x, "tok", [(z * Y + y, z * Y + (y + distance) % Y) for z in range(Z) for y in range(Y)]
    )


def vmem(n):
    return [pl.BlockSpec(memory_space=pltpu.VMEM)] * n


def smem():
    return pl.BlockSpec(memory_space=pltpu.SMEM)


def params():
    return pltpu.CompilerParams(vmem_limit_bytes=56 << 20)


def project_kernel(
    fids, x0, p0, m0, q0, r0, x1, pm1, qr1, weight, cosine, sine, ids,
    queries, message, normed, held, mixed, sems,
):
    fetches = []
    for i in range(3):
        part = slice(i * 256, (i + 1) * 256)
        fetches.append(pltpu.make_async_copy(weight.at[:, part], held.at[i], sems.at[i]))
    for fetch in fetches:
        fetch.start()
    pieces = []
    rows = T + 16
    mine = ((x0, 0), (p0, 0), (m0, 0), (q0, 0), (r0, 0))
    theirs = ((x1, 0), (pm1, 0), (pm1, rows), (qr1, 0), (qr1, HALF))
    for *three, (q, top), (r, bottom) in (mine, theirs):
        for ref, base in three:
            pieces.append(((ref, base), (ref, base + HALF), (ref, base + T)))
        pieces.append(((q, top), (r, bottom), (r, bottom + HALF)))
    step_rows = 16
    for half in range(2):

        def step(i, _):
            row = pl.multiple_of(i * step_rows, step_rows)
            total = jnp.zeros((step_rows, PIECE), f32)
            for piece in pieces:
                ref, base = piece[half]
                v = ref[pl.ds(base + row, step_rows), :].astype(f32)
                total += v * v
            mean = jnp.sum(total, axis=1, keepdims=True) * (1.0 / MODEL_WIDTH)
            scale = lax.rsqrt(mean + epsilon)
            for k, piece in enumerate(pieces):
                ref, base = piece[half]
                gain_ref, gain_base = piece[2]
                gain = gain_ref[gain_base : gain_base + 16, :].astype(f32)
                v = ref[pl.ds(base + row, step_rows), :].astype(f32) * scale * gain
                column = pl.multiple_of(fids[k] * PIECE, PIECE)
                normed[pl.ds(half * HALF + row, step_rows), pl.ds(column, PIECE)] = v.astype(bf16)
            return 0

        lax.fori_loop(0, HALF // step_rows, step, 0, unroll=4)

    def columns(i, _):
        for j in range(3):
            pl.when(i == j)(fetches[j].wait)
        at = pl.multiple_of(i * 256, 256)
        mixed[:, pl.ds(at, 256)] = jnp.dot(normed[...], held[i], preferred_element_type=f32)
        return 0

    lax.fori_loop(0, (GROUP + 2) * HEAD_SIZE // 256, columns, 0)

    def rotated(h):
        v = mixed[:, h * HEAD_SIZE : (h + 1) * HEAD_SIZE]
        return v * cosine[...] + pltpu.roll(v, HEAD_SIZE // 2, 1) * sine[...]

    for h in range(GROUP):
        queries[h * HEAD_SIZE : (h + 1) * HEAD_SIZE, :] = rotated(h).astype(bf16).T
    message[0:T, :] = rotated(GROUP).astype(bf16)
    for j in range(T // LANES):
        v = mixed[j * LANES : (j + 1) * LANES, (GROUP + 1) * HEAD_SIZE :]
        message[T + j * LANES : T + (j + 1) * LANES, :] = v.astype(bf16).T
    message[KV_ROWS:MSG_ROWS, :] = ids[...]


def project(fids, pieces, weight, cosine, sine, ids):
    width = (GROUP + 2) * HEAD_SIZE
    return pl.pallas_call(
        project_kernel,
        out_shape=(
            jax.ShapeDtypeStruct((GROUP * HEAD_SIZE, T), bf16),
            jax.ShapeDtypeStruct((MSG_ROWS, LANES), bf16),
        ),
        in_specs=[smem()] + vmem(8) + [pl.BlockSpec(memory_space=pl.ANY)] + vmem(3),
        out_specs=tuple(vmem(2)),
        scratch_shapes=[
            pltpu.VMEM((T, MODEL_WIDTH), bf16),
            pltpu.VMEM((3, MODEL_WIDTH, 256), bf16),
            pltpu.VMEM((T, width), f32),
            pltpu.SemaphoreType.DMA((3,)),
        ],
        compiler_params=params(),
        cost_estimate=pl.CostEstimate(
            flops=2 * T * MODEL_WIDTH * width, transcendentals=0, bytes_accessed=12 << 20
        ),
        name="project",
    )(fids, *pieces, weight, cosine, sine, ids)


def attend_block(block, queries, highest, totals, accum, change, together):
    keys = block[0:T, :]
    values = jnp.concatenate(
        [block[T + j * LANES : T + (j + 1) * LANES, :] for j in range(T // LANES)], axis=1
    )

    def head(h):
        rows = pl.ds(pl.multiple_of(h * HEAD_SIZE, HEAD_SIZE), HEAD_SIZE)
        for at in range(0, T, LANES):
            part = slice(at, at + LANES)
            scores = jnp.dot(keys, queries[rows, part], preferred_element_type=f32)
            scores = change(scores, at)
            old = highest[h, :, part]
            new = jnp.maximum(old, jnp.max(scores, axis=0, keepdims=True))
            weights = jnp.exp2((scores - new) * exponent_scale)
            fade = jnp.exp2((old - new) * exponent_scale)
            highest[h, :, part] = new
            totals[h, :, part] = totals[h, :, part] * fade + jnp.sum(weights, axis=0, keepdims=True)
            accum[rows, part] = accum[rows, part] * fade + jnp.dot(
                values, weights.astype(bf16), preferred_element_type=f32
            )

    def heads(i, _):
        for j in range(together):
            head(i * together + j)
        return 0

    lax.fori_loop(0, GROUP // together, heads, 0)


def clear(highest, totals, accum):
    highest[...] = jnp.full(highest.shape, floor_score, f32)
    totals[...] = jnp.zeros(totals.shape, f32)
    accum[...] = jnp.zeros(accum.shape, f32)


def whole_of(ref):
    def copies(block, sems):
        return [pltpu.make_async_copy(ref.at[pl.ds(0, MSG_ROWS)], block, sems.at[0])]

    return copies


def pair_of(keys, base, values, value_base):
    rest = MSG_ROWS - T

    def copies(block, sems):
        return [
            pltpu.make_async_copy(keys.at[pl.ds(base, T)], block.at[pl.ds(0, T)], sems.at[0]),
            pltpu.make_async_copy(
                values.at[pl.ds(value_base, rest)], block.at[pl.ds(T, rest)], sems.at[1]
            ),
        ]

    return copies


def attend_earlier(info, indices, sources, queries, blocks, bias, sems, fill, state):
    own, first_doc = info[0], info[1].astype(f32)

    def reached(j):
        return (indices[j] >= 0) & (indices[j] < own)

    def each(j, act):
        def run():
            for copy in sources[j](blocks.at[j], sems.at[j]):
                act(copy)

        return run

    for j in range(len(indices)):
        pl.when(reached(j))(each(j, lambda copy: copy.start()))
    fill()

    def step(k, _):
        wanted = reached(0)
        for j in range(1, len(indices)):
            wanted = jnp.where(k == j, reached(j), wanted)

        @pl.when(wanted)
        def _():
            for j in range(len(indices)):
                pl.when(k == j)(each(j, lambda copy: copy.wait()))
            block = blocks.at[k]
            ids = block[KV_ROWS:MSG_ROWS, :].astype(f32)
            low = jnp.sum(jnp.where(ids < first_doc, 1.0, 0.0)).astype(jnp.int32)

            @pl.when(low < T)
            def _():
                key = lax.broadcasted_iota(jnp.int32, (T, LANES), 0)
                bias[...] = jnp.where(key < low, floor_score, 0.0)
                attend_block(block, queries, *state, lambda scores, at: scores + bias[...], TOGETHER)

        return 0

    lax.fori_loop(0, len(indices), step, 0)


TOGETHER = 4
STATE = (
    jax.ShapeDtypeStruct((GROUP, 1, T), f32),
    jax.ShapeDtypeStruct((GROUP, 1, T), f32),
    jax.ShapeDtypeStruct((GROUP * HEAD_SIZE, T), f32),
)
BLOCK_FLOPS = 4 * GROUP * T * T * HEAD_SIZE


def earlier_scratch(n):
    return [
        pltpu.VMEM((n, MSG_ROWS, LANES), bf16),
        pltpu.VMEM((T, LANES), f32),
        pltpu.SemaphoreType.DMA((n, 2)),
    ]


def attend_first(queries, message, doc_rows, doc_columns):
    def kernel(message, queries, doc_rows, doc_columns, *state):
        clear(*state)

        def change(scores, at):
            key = lax.broadcasted_iota(jnp.int32, scores.shape, 0)
            query = lax.broadcasted_iota(jnp.int32, scores.shape, 1) + at
            same = doc_rows[...] == doc_columns[0:1, at : at + LANES]
            return jnp.where((key <= query) & same, scores, floor_score)

        attend_block(message, queries, *state, change, 1)

    return pl.pallas_call(
        kernel,
        out_shape=STATE,
        in_specs=vmem(4),
        out_specs=tuple(vmem(3)),
        compiler_params=params(),
        cost_estimate=pl.CostEstimate(
            flops=2 * BLOCK_FLOPS, transcendentals=GROUP * T * T, bytes_accessed=2 << 20
        ),
        name="attend_own",
    )(message, queries, doc_rows, doc_columns)


def attend_stage(number, info, queries, state, along, against, straight):
    n = 2 + (straight is not None)

    def kernel(number, info, queries, *refs):
        messages, old, new, refs = refs[:n], refs[n : n + 3], refs[n + 3 : n + 6], refs[n + 6 :]

        def fill():
            for a, b in zip(old, new):
                b[...] = a[...]

        s = number[0]
        two_away = info[jnp.maximum(3 + 4 * s - 2, 3)]
        indices = [info[3 + 4 * s + 3], info[3 + 4 * s + 1]]
        indices.append(jnp.where(s > 0, two_away, -1))
        sources = [whole_of(messages[0]), whole_of(messages[1])]
        sources.append(pair_of(messages[0], MSG_ROWS, messages[1], MSG_ROWS))
        if straight is not None:
            indices.append(info[3 + 4 * s + 4])
            sources.append(whole_of(messages[2]))
        attend_earlier(info, indices, sources, queries, *refs, fill, new)

    messages = [along, against] + ([straight] if straight is not None else [])
    return pl.pallas_call(
        kernel,
        out_shape=STATE,
        in_specs=[smem(), smem()]
        + vmem(1)
        + [pl.BlockSpec(memory_space=pl.ANY)] * n
        + vmem(3),
        out_specs=tuple(vmem(3)),
        scratch_shapes=earlier_scratch(1 + n),
        input_output_aliases={3 + n + i: i for i in range(3)},
        compiler_params=params(),
        cost_estimate=pl.CostEstimate(
            flops=2 * (1 + n) * BLOCK_FLOPS,
            transcendentals=(1 + n) * GROUP * T * T,
            bytes_accessed=3 << 20,
        ),
        name="attend_stage",
    )(number, info, queries, *messages, *state)


def fetch_columns(columns, first, count, weight, held, sems):
    fetches = []
    for k in range(count):
        at = pl.multiple_of(columns[first + k] * PIECE, PIECE)
        fetches.append(pltpu.make_async_copy(weight.at[:, pl.ds(at, PIECE)], held.at[k], sems.at[k]))
    for fetch in fetches:
        fetch.start()
    return fetches


def column_scratch(count):
    return [
        pltpu.VMEM((count, GROUP * HEAD_SIZE, PIECE), bf16),
        pltpu.SemaphoreType.DMA((count,)),
    ]


def finish(info, queries, own_state, state, keys, values, columns, weight):
    def kernel(
        info, columns, queries, keys, values, own_highest, own_totals, own_accum,
        old_highest, old_totals, old_accum, weight,
        heads, first, far, highest, totals, accum, blocks, bias, sems, held, held_sems,
    ):
        fetches = fetch_columns(columns, 0, 2, weight, held, held_sems)

        def fill():
            highest[...] = old_highest[...]
            totals[...] = old_totals[...]
            accum[...] = old_accum[...]

        attend_earlier(
            info, [info[3 + 4 * 4 + 2]], [pair_of(keys, 0, values, 0)], queries, blocks, bias, sems, fill,
            (highest, totals, accum),
        )
        query = lax.broadcasted_iota(jnp.int32, (1, T), 1)
        for h in range(GROUP):
            rows = slice(h * HEAD_SIZE, (h + 1) * HEAD_SIZE)
            used = (query < info[2]) & (totals[h] > 0.0)
            near, past = own_highest[h], highest[h]
            top = jnp.where(used, jnp.maximum(near, past), near)
            near = jnp.exp2((near - top) * exponent_scale)
            past = jnp.where(used, jnp.exp2((past - top) * exponent_scale), 0.0)
            total = own_totals[h] * near + totals[h] * past
            summed = own_accum[rows, :] * near + accum[rows, :] * past
            heads[:, rows] = (summed / total).astype(bf16).T
        for fetch in fetches:
            fetch.wait()
        first[...] = jnp.dot(heads[...], held[0], preferred_element_type=f32).astype(bf16)
        far[...] = jnp.dot(heads[...], held[1], preferred_element_type=f32)

    return pl.pallas_call(
        kernel,
        out_shape=(
            jax.ShapeDtypeStruct((T, GROUP * HEAD_SIZE), bf16),
            jax.ShapeDtypeStruct((T, PIECE), bf16),
            jax.ShapeDtypeStruct((T, PIECE), f32),
        ),
        in_specs=[smem(), smem()]
        + vmem(1)
        + [pl.BlockSpec(memory_space=pl.ANY)] * 2
        + vmem(6)
        + [pl.BlockSpec(memory_space=pl.ANY)],
        out_specs=tuple(vmem(3)),
        scratch_shapes=[
            pltpu.VMEM((GROUP, 1, T), f32),
            pltpu.VMEM((GROUP, 1, T), f32),
            pltpu.VMEM((GROUP * HEAD_SIZE, T), f32),
        ]
        + earlier_scratch(1)
        + column_scratch(2),
        compiler_params=params(),
        cost_estimate=pl.CostEstimate(
            flops=2 * T * T * MODEL_WIDTH, transcendentals=0, bytes_accessed=8 << 20
        ),
        name="finish",
    )(info, columns, queries, keys, values, *own_state, *state, weight)


def three_products(columns, start, heads, weight, dtype):
    def kernel(columns, heads, weight, out, held, sems):
        fetches = fetch_columns(columns, start, 3, weight, held, sems)

        def multiply(k, _):
            for j in range(3):
                pl.when(k == j)(fetches[j].wait)
            out[k] = jnp.dot(heads[...], held[k], preferred_element_type=f32).astype(dtype)
            return 0

        lax.fori_loop(0, 3, multiply, 0)

    return pl.pallas_call(
        kernel,
        out_shape=jax.ShapeDtypeStruct((3, T, PIECE), dtype),
        in_specs=[smem()] + vmem(1) + [pl.BlockSpec(memory_space=pl.ANY)],
        out_specs=vmem(1)[0],
        scratch_shapes=column_scratch(3),
        compiler_params=params(),
        cost_estimate=pl.CostEstimate(
            flops=2 * T * T * MODEL_WIDTH // 2, transcendentals=0, bytes_accessed=6 << 20
        ),
        name="three_products",
    )(columns, heads, weight)


def body(tokens, norm_gain, query_key_value_weight, out_weight, doc_ids):
    shard = lax.axis_index("tok")
    chip = lax.axis_index("head")
    core = lax.axis_index("grp")
    row, column = shard // Y, shard % Y

    own = jnp.concatenate([tokens, jnp.broadcast_to(norm_gain[None, :], (16, PIECE))], axis=0)
    behind = shift(own, "head", 1)
    ahead = shift(own, "head", -1)
    across = shift(own, "grp", 1)
    chips = jnp.stack([chip, (chip - 1) % 4, (chip + 1) % 4, (chip + 2) % 4])
    fids = jnp.concatenate([chips * 2 + core, chips * 2 + 1 - core]).astype(jnp.int32)

    positions = shard * T + jnp.arange(T, dtype=jnp.int32)
    half = HEAD_SIZE // 2
    inverse = 1.0 / theta ** (jnp.arange(half, dtype=f32) * (2.0 / HEAD_SIZE))
    angles = positions.astype(f32)[:, None] * inverse[None, :]
    cosine, sine = jnp.cos(angles), jnp.sin(angles)
    cosine = jnp.concatenate([cosine, cosine], axis=1)
    sine = jnp.concatenate([-sine, sine], axis=1)
    ids = jnp.concatenate(
        [doc_ids.reshape(T // LANES, LANES), jnp.full((16 - T // LANES, LANES), 99, jnp.int32)]
    ).astype(bf16)
    doc_rows = jnp.broadcast_to(doc_ids.astype(f32)[:, None], (T, LANES))
    doc_columns = jnp.broadcast_to(doc_ids.astype(f32)[None, :], (8, T))

    blocks = [4 * (row - s) + (column + k) % Y for s in range(5) for k in range(4)]
    info = jnp.stack(
        [shard, doc_ids[0], jnp.sum((doc_ids == doc_ids[0]).astype(jnp.int32))] + blocks
    ).astype(jnp.int32)
    order = jnp.stack([(chip + 2) % 4, (chip + 1) % 4, (chip + 3) % 4, chip])
    columns = jnp.concatenate(
        [order[:1] * 2 + 1 - core, order[:1] * 2 + core, order[1:] * 2 + 1 - core, order[1:] * 2 + core]
    ).astype(jnp.int32)

    behind, ahead, across, fids, info, columns, cosine, sine, ids = lax.optimization_barrier(
        (behind, ahead, across, fids, info, columns, cosine, sine, ids)
    )
    top = shift(behind[:HALF], "head", 1)
    bottom = shift(ahead[HALF:], "head", -1)
    across_near = shift(jnp.concatenate([behind, ahead]), "grp", 1)
    top, bottom, doc_rows, doc_columns = lax.optimization_barrier(
        (top, bottom, doc_rows, doc_columns)
    )
    mine = [own, behind, ahead, top, bottom]
    across_far = shift(jnp.concatenate([top, bottom]), "grp", 1)
    theirs = [across, across_near, across_far]
    queries, message = project(fids, mine + theirs, query_key_value_weight, cosine, sine, ids)

    state = (
        jnp.full((GROUP, 1, T), floor_score, f32),
        jnp.zeros((GROUP, 1, T), f32),
        jnp.zeros((GROUP * HEAD_SIZE, T), f32),
    )
    along, against = shift_y(message, 1), shift_y(message, -1)
    straight = shift_z(message)
    own_state = attend_first(queries, message, doc_rows, doc_columns)
    along = jnp.pad(along, ((0, T), (0, 0)))
    against = jnp.pad(against, ((0, MSG_ROWS - T), (0, 0)))

    def stage(s, carried):
        along, against, straight, state = carried
        next_along = shift_y(jnp.concatenate([straight, along[:T]]), 1)
        next_against = shift_y(jnp.concatenate([straight, against[T:MSG_ROWS]]), -1)
        following = shift_z(straight)
        number = jnp.full((1,), s - 1, jnp.int32)
        state = attend_stage(number, info, queries, state, along, against, straight)
        return next_along, next_against, following, state

    along, against, straight, state = lax.fori_loop(
        1, 5, stage, (along, against, straight, state)
    )
    keys = shift_y(along[:T], 1)
    values = shift_y(against[T:MSG_ROWS], -1)
    state = attend_stage(
        jnp.full((1,), 4, jnp.int32), info, queries, state, along, against, None
    )

    heads, first, products = finish(
        info, queries, own_state, state, keys, values, columns, out_weight
    )
    first = shift(first, "grp", 1)
    others = three_products(columns, 2, heads, out_weight, bf16)
    others = shift(others, "grp", 1)

    far = (products + first.astype(f32)).astype(bf16)
    far_up = shift(far[:HALF], "head", 1)
    far_down = shift(far[HALF:], "head", -1)
    heads, far = lax.optimization_barrier((heads, far))
    products = three_products(columns, 5, heads, out_weight, f32)
    up_low = (products[0, HALF:] + others[0, HALF:].astype(f32)).astype(bf16)
    down_high = (products[1, :HALF] + others[1, :HALF].astype(f32)).astype(bf16)
    up_low = shift(up_low, "head", 1)
    down_high = shift(down_high, "head", -1)
    up_high = products[0, :HALF] + others[0, :HALF].astype(f32) + far_up.astype(f32)
    down_low = products[1, HALF:] + others[1, HALF:].astype(f32) + far_down.astype(f32)
    up_high = shift(up_high.astype(bf16), "head", 1)
    down_low = shift(down_low.astype(bf16), "head", -1)
    kept = products[2] + others[2].astype(f32)
    return jnp.concatenate(
        [
            kept[:HALF] + up_high.astype(f32) + down_high.astype(f32),
            kept[HALF:] + up_low.astype(f32) + down_low.astype(f32),
        ]
    ).astype(bf16)


def solution(mesh):
    return jax.shard_map(
        body,
        mesh=mesh,
        in_specs=(
            P("tok", ("head", "grp")),
            P(("head", "grp")),
            P(None, ("head", "grp")),
            P(("head", "grp"), None),
            P("tok"),
        ),
        out_specs=P("tok", ("head", "grp")),
        check_vma=False,
    )
```

```python
import jax
import jax.numpy as jnp
from jax import lax
from jax.experimental import pallas as pl
from jax.experimental.pallas import tpu as pltpu
from jax.sharding import PartitionSpec as P


QUERY_HEADS = 32
KEY_VALUE_HEADS = 8
HEAD_SIZE = 128
GROUP = QUERY_HEADS // KEY_VALUE_HEADS
MODEL_WIDTH = 4096

T = 512
HALF = T // 2
PIECE = 512
Y, Z = 4, 8
LANES = 128
KV_ROWS = 2 * T
MSG_ROWS = KV_ROWS + 16

epsilon = 1e-05
theta = 500000.0
floor_score = -1e30
exponent_scale = HEAD_SIZE**-0.5 * 1.4426950408889634

bf16 = jnp.bfloat16
f32 = jnp.float32


def shift(x, axis, distance):
    n = lax.axis_size(axis)
    return lax.ppermute(x, axis, [(i, (i + distance) % n) for i in range(n)])


def shift_z(x):
    return lax.ppermute(
        x, "tok", [(z * Y + y, (z + 1) % Z * Y + y) for z in range(Z) for y in range(Y)]
    )


def shift_y(x, distance):
    return lax.ppermute(
        x, "tok", [(z * Y + y, z * Y + (y + distance) % Y) for z in range(Z) for y in range(Y)]
    )


def vmem(n):
    return [pl.BlockSpec(memory_space=pltpu.VMEM)] * n


def smem():
    return pl.BlockSpec(memory_space=pltpu.SMEM)


def params():
    return pltpu.CompilerParams(vmem_limit_bytes=56 << 20)


def project_kernel(
    fids, x0, p0, m0, q0, r0, x1, pm1, qr1, weight, cosine, sine, ids,
    queries, message, normed, held, mixed, sems,
):
    fetches = []
    for i in range(3):
        part = slice(i * 256, (i + 1) * 256)
        fetches.append(pltpu.make_async_copy(weight.at[:, part], held.at[i], sems.at[i]))
    for fetch in fetches:
        fetch.start()
    pieces = []
    rows = T + 16
    mine = ((x0, 0), (p0, 0), (m0, 0), (q0, 0), (r0, 0))
    theirs = ((x1, 0), (pm1, 0), (pm1, rows), (qr1, 0), (qr1, HALF))
    for *three, (q, top), (r, bottom) in (mine, theirs):
        for ref, base in three:
            pieces.append(((ref, base), (ref, base + HALF), (ref, base + T)))
        pieces.append(((q, top), (r, bottom), (r, bottom + HALF)))
    step_rows = 16
    for half in range(2):

        def step(i, _):
            row = pl.multiple_of(i * step_rows, step_rows)
            total = jnp.zeros((step_rows, PIECE), f32)
            for piece in pieces:
                ref, base = piece[half]
                v = ref[pl.ds(base + row, step_rows), :].astype(f32)
                total += v * v
            mean = jnp.sum(total, axis=1, keepdims=True) * (1.0 / MODEL_WIDTH)
            scale = lax.rsqrt(mean + epsilon)
            for k, piece in enumerate(pieces):
                ref, base = piece[half]
                gain_ref, gain_base = piece[2]
                gain = gain_ref[gain_base : gain_base + 16, :].astype(f32)
                v = ref[pl.ds(base + row, step_rows), :].astype(f32) * scale * gain
                column = pl.multiple_of(fids[k] * PIECE, PIECE)
                normed[pl.ds(half * HALF + row, step_rows), pl.ds(column, PIECE)] = v.astype(bf16)
            return 0

        lax.fori_loop(0, HALF // step_rows, step, 0, unroll=4)

    def columns(i, _):
        for j in range(3):
            pl.when(i == j)(fetches[j].wait)
        at = pl.multiple_of(i * 256, 256)
        mixed[:, pl.ds(at, 256)] = jnp.dot(normed[...], held[i], preferred_element_type=f32)
        return 0

    lax.fori_loop(0, (GROUP + 2) * HEAD_SIZE // 256, columns, 0)

    def rotated(h):
        v = mixed[:, h * HEAD_SIZE : (h + 1) * HEAD_SIZE]
        return v * cosine[...] + pltpu.roll(v, HEAD_SIZE // 2, 1) * sine[...]

    for h in range(GROUP):
        queries[h * HEAD_SIZE : (h + 1) * HEAD_SIZE, :] = rotated(h).astype(bf16).T
    message[0:T, :] = rotated(GROUP).astype(bf16)
    for j in range(T // LANES):
        v = mixed[j * LANES : (j + 1) * LANES, (GROUP + 1) * HEAD_SIZE :]
        message[T + j * LANES : T + (j + 1) * LANES, :] = v.astype(bf16).T
    message[KV_ROWS:MSG_ROWS, :] = ids[...]


def project(fids, pieces, weight, cosine, sine, ids):
    width = (GROUP + 2) * HEAD_SIZE
    return pl.pallas_call(
        project_kernel,
        out_shape=(
            jax.ShapeDtypeStruct((GROUP * HEAD_SIZE, T), bf16),
            jax.ShapeDtypeStruct((MSG_ROWS, LANES), bf16),
        ),
        in_specs=[smem()] + vmem(8) + [pl.BlockSpec(memory_space=pl.ANY)] + vmem(3),
        out_specs=tuple(vmem(2)),
        scratch_shapes=[
            pltpu.VMEM((T, MODEL_WIDTH), bf16),
            pltpu.VMEM((3, MODEL_WIDTH, 256), bf16),
            pltpu.VMEM((T, width), f32),
            pltpu.SemaphoreType.DMA((3,)),
        ],
        compiler_params=params(),
        cost_estimate=pl.CostEstimate(
            flops=2 * T * MODEL_WIDTH * width, transcendentals=0, bytes_accessed=12 << 20
        ),
        name="project",
    )(fids, *pieces, weight, cosine, sine, ids)


def attend_block(block, queries, highest, totals, accum, change, together):
    keys = block[0:T, :]
    values = jnp.concatenate(
        [block[T + j * LANES : T + (j + 1) * LANES, :] for j in range(T // LANES)], axis=1
    )

    def head(h):
        rows = pl.ds(pl.multiple_of(h * HEAD_SIZE, HEAD_SIZE), HEAD_SIZE)
        for at in range(0, T, LANES):
            part = slice(at, at + LANES)
            scores = jnp.dot(keys, queries[rows, part], preferred_element_type=f32)
            scores = change(scores, at)
            old = highest[h, :, part]
            new = jnp.maximum(old, jnp.max(scores, axis=0, keepdims=True))
            weights = jnp.exp2((scores - new) * exponent_scale)
            fade = jnp.exp2((old - new) * exponent_scale)
            highest[h, :, part] = new
            totals[h, :, part] = totals[h, :, part] * fade + jnp.sum(weights, axis=0, keepdims=True)
            accum[rows, part] = accum[rows, part] * fade + jnp.dot(
                values, weights.astype(bf16), preferred_element_type=f32
            )

    def heads(i, _):
        for j in range(together):
            head(i * together + j)
        return 0

    lax.fori_loop(0, GROUP // together, heads, 0)


def clear(highest, totals, accum):
    highest[...] = jnp.full(highest.shape, floor_score, f32)
    totals[...] = jnp.zeros(totals.shape, f32)
    accum[...] = jnp.zeros(accum.shape, f32)


def whole_of(ref):
    def copies(block, sems):
        return [pltpu.make_async_copy(ref.at[pl.ds(0, MSG_ROWS)], block, sems.at[0])]

    return copies


def pair_of(keys, base, values, value_base):
    rest = MSG_ROWS - T

    def copies(block, sems):
        return [
            pltpu.make_async_copy(keys.at[pl.ds(base, T)], block.at[pl.ds(0, T)], sems.at[0]),
            pltpu.make_async_copy(
                values.at[pl.ds(value_base, rest)], block.at[pl.ds(T, rest)], sems.at[1]
            ),
        ]

    return copies


def attend_earlier(info, indices, sources, queries, blocks, bias, sems, fill, state):
    own, first_doc = info[0], info[1].astype(f32)

    def reached(j):
        return (indices[j] >= 0) & (indices[j] < own)

    def each(j, act):
        def run():
            for copy in sources[j](blocks.at[j], sems.at[j]):
                act(copy)

        return run

    for j in range(len(indices)):
        pl.when(reached(j))(each(j, lambda copy: copy.start()))
    fill()

    def step(k, _):
        wanted = reached(0)
        for j in range(1, len(indices)):
            wanted = jnp.where(k == j, reached(j), wanted)

        @pl.when(wanted)
        def _():
            for j in range(len(indices)):
                pl.when(k == j)(each(j, lambda copy: copy.wait()))
            block = blocks.at[k]
            ids = block[KV_ROWS:MSG_ROWS, :].astype(f32)
            low = jnp.sum(jnp.where(ids < first_doc, 1.0, 0.0)).astype(jnp.int32)

            @pl.when(low < T)
            def _():
                key = lax.broadcasted_iota(jnp.int32, (T, LANES), 0)
                bias[...] = jnp.where(key < low, floor_score, 0.0)
                attend_block(block, queries, *state, lambda scores, at: scores + bias[...], TOGETHER)

        return 0

    lax.fori_loop(0, len(indices), step, 0)


TOGETHER = 4
STATE = (
    jax.ShapeDtypeStruct((GROUP, 1, T), f32),
    jax.ShapeDtypeStruct((GROUP, 1, T), f32),
    jax.ShapeDtypeStruct((GROUP * HEAD_SIZE, T), f32),
)
BLOCK_FLOPS = 4 * GROUP * T * T * HEAD_SIZE


def earlier_scratch(n):
    return [
        pltpu.VMEM((n, MSG_ROWS, LANES), bf16),
        pltpu.VMEM((T, LANES), f32),
        pltpu.SemaphoreType.DMA((n, 2)),
    ]


def attend_first(queries, message, doc_rows, doc_columns):
    def kernel(message, queries, doc_rows, doc_columns, *states):
        state = states[:3]
        clear(*state)
        clear(*states[3:])

        def change(scores, at):
            key = lax.broadcasted_iota(jnp.int32, scores.shape, 0)
            query = lax.broadcasted_iota(jnp.int32, scores.shape, 1) + at
            same = doc_rows[...] == doc_columns[0:1, at : at + LANES]
            return jnp.where((key <= query) & same, scores, floor_score)

        attend_block(message, queries, *state, change, 1)

    made = pl.pallas_call(
        kernel,
        out_shape=STATE + STATE,
        in_specs=vmem(4),
        out_specs=tuple(vmem(6)),
        compiler_params=params(),
        cost_estimate=pl.CostEstimate(
            flops=2 * BLOCK_FLOPS, transcendentals=GROUP * T * T, bytes_accessed=2 << 20
        ),
        name="attend_own",
    )(message, queries, doc_rows, doc_columns)
    return made[:3], made[3:]


def attend_stage(number, info, queries, state, along, against, straight):
    n = 2 + (straight is not None)

    def kernel(number, info, queries, *refs):
        messages, old, new, refs = refs[:n], refs[n : n + 3], refs[n + 3 : n + 6], refs[n + 6 :]

        def fill():
            for a, b in zip(old, new):
                b[...] = a[...]

        s = number[0]
        two_away = info[jnp.maximum(3 + 4 * s - 2, 3)]
        indices = [info[3 + 4 * s + 3], info[3 + 4 * s + 1]]
        indices.append(jnp.where(s > 0, two_away, -1))
        sources = [whole_of(messages[0]), whole_of(messages[1])]
        sources.append(pair_of(messages[0], MSG_ROWS, messages[1], MSG_ROWS))
        if straight is not None:
            indices.append(info[3 + 4 * s + 4])
            sources.append(whole_of(messages[2]))
        attend_earlier(info, indices, sources, queries, *refs, fill, new)

    messages = [along, against] + ([straight] if straight is not None else [])
    return pl.pallas_call(
        kernel,
        out_shape=STATE,
        in_specs=[smem(), smem()]
        + vmem(1)
        + [pl.BlockSpec(memory_space=pl.ANY)] * n
        + vmem(3),
        out_specs=tuple(vmem(3)),
        scratch_shapes=earlier_scratch(1 + n),
        input_output_aliases={3 + n + i: i for i in range(3)},
        compiler_params=params(),
        cost_estimate=pl.CostEstimate(
            flops=2 * (1 + n) * BLOCK_FLOPS,
            transcendentals=(1 + n) * GROUP * T * T,
            bytes_accessed=3 << 20,
        ),
        name="attend_stage",
    )(number, info, queries, *messages, *state)


def fetch_columns(columns, first, count, weight, held, sems):
    fetches = []
    for k in range(count):
        at = pl.multiple_of(columns[first + k] * PIECE, PIECE)
        fetches.append(pltpu.make_async_copy(weight.at[:, pl.ds(at, PIECE)], held.at[k], sems.at[k]))
    for fetch in fetches:
        fetch.start()
    return fetches


def column_scratch(count):
    return [
        pltpu.VMEM((count, GROUP * HEAD_SIZE, PIECE), bf16),
        pltpu.SemaphoreType.DMA((count,)),
    ]


def finish(info, queries, own_state, state, keys, values, columns, weight):
    def kernel(
        info, columns, queries, keys, values, own_highest, own_totals, own_accum,
        old_highest, old_totals, old_accum, weight,
        first, others, products, highest, totals, accum, blocks, bias, sems, held, held_sems, heads,
    ):
        fetches = fetch_columns(columns, 0, 8, weight, held, held_sems)

        def fill():
            highest[...] = old_highest[...]
            totals[...] = old_totals[...]
            accum[...] = old_accum[...]

        attend_earlier(
            info, [info[3 + 4 * 4 + 2]], [pair_of(keys, 0, values, 0)], queries, blocks, bias, sems, fill,
            (highest, totals, accum),
        )
        query = lax.broadcasted_iota(jnp.int32, (1, T), 1)
        for h in range(GROUP):
            rows = slice(h * HEAD_SIZE, (h + 1) * HEAD_SIZE)
            used = (query < info[2]) & (totals[h] > 0.0)
            near, past = own_highest[h], highest[h]
            top = jnp.where(used, jnp.maximum(near, past), near)
            near = jnp.exp2((near - top) * exponent_scale)
            past = jnp.where(used, jnp.exp2((past - top) * exponent_scale), 0.0)
            total = own_totals[h] * near + totals[h] * past
            summed = own_accum[rows, :] * near + accum[rows, :] * past
            heads[:, rows] = (summed / total).astype(bf16).T
        for fetch in fetches:
            fetch.wait()

        def product(k):
            return jnp.dot(heads[...], held[k], preferred_element_type=f32)

        first[...] = product(0).astype(bf16)

        def partner(k, _):
            others[k] = product(1 + k).astype(bf16)
            return 0

        def kept(k, _):
            products[k] = product(4 + k)
            return 0

        lax.fori_loop(0, 3, partner, 0)
        lax.fori_loop(0, 4, kept, 0)

    return pl.pallas_call(
        kernel,
        out_shape=(
            jax.ShapeDtypeStruct((T, PIECE), bf16),
            jax.ShapeDtypeStruct((3, T, PIECE), bf16),
            jax.ShapeDtypeStruct((4, T, PIECE), f32),
        ),
        in_specs=[smem(), smem()]
        + vmem(1)
        + [pl.BlockSpec(memory_space=pl.ANY)] * 2
        + vmem(6)
        + [pl.BlockSpec(memory_space=pl.ANY)],
        out_specs=tuple(vmem(3)),
        scratch_shapes=[
            pltpu.VMEM((GROUP, 1, T), f32),
            pltpu.VMEM((GROUP, 1, T), f32),
            pltpu.VMEM((GROUP * HEAD_SIZE, T), f32),
        ]
        + earlier_scratch(1)
        + column_scratch(8)
        + [pltpu.VMEM((T, GROUP * HEAD_SIZE), bf16)],
        compiler_params=params(),
        cost_estimate=pl.CostEstimate(
            flops=2 * T * T * MODEL_WIDTH, transcendentals=0, bytes_accessed=8 << 20
        ),
        name="finish",
    )(info, columns, queries, keys, values, *own_state, *state, weight)


def body(tokens, norm_gain, query_key_value_weight, out_weight, doc_ids):
    shard = lax.axis_index("tok")
    chip = lax.axis_index("head")
    core = lax.axis_index("grp")
    row, column = shard // Y, shard % Y

    own = jnp.concatenate([tokens, jnp.broadcast_to(norm_gain[None, :], (16, PIECE))], axis=0)
    behind = shift(own, "head", 1)
    ahead = shift(own, "head", -1)
    across = shift(own, "grp", 1)
    chips = jnp.stack([chip, (chip - 1) % 4, (chip + 1) % 4, (chip + 2) % 4])
    fids = jnp.concatenate([chips * 2 + core, chips * 2 + 1 - core]).astype(jnp.int32)

    positions = shard * T + jnp.arange(T, dtype=jnp.int32)
    half = HEAD_SIZE // 2
    inverse = 1.0 / theta ** (jnp.arange(half, dtype=f32) * (2.0 / HEAD_SIZE))
    angles = positions.astype(f32)[:, None] * inverse[None, :]
    cosine, sine = jnp.cos(angles), jnp.sin(angles)
    cosine = jnp.concatenate([cosine, cosine], axis=1)
    sine = jnp.concatenate([-sine, sine], axis=1)
    ids = jnp.concatenate(
        [doc_ids.reshape(T // LANES, LANES), jnp.full((16 - T // LANES, LANES), 99, jnp.int32)]
    ).astype(bf16)
    doc_rows = jnp.broadcast_to(doc_ids.astype(f32)[:, None], (T, LANES))
    doc_columns = jnp.broadcast_to(doc_ids.astype(f32)[None, :], (8, T))

    blocks = [4 * (row - s) + (column + k) % Y for s in range(5) for k in range(4)]
    info = jnp.stack(
        [shard, doc_ids[0], jnp.sum((doc_ids == doc_ids[0]).astype(jnp.int32))] + blocks
    ).astype(jnp.int32)
    order = jnp.stack([(chip + 2) % 4, (chip + 1) % 4, (chip + 3) % 4, chip])
    columns = jnp.concatenate([order * 2 + 1 - core, order * 2 + core]).astype(jnp.int32)

    tables = (fids, info, columns, cosine, sine, ids, doc_rows, doc_columns)
    behind, ahead, across, tables = lax.optimization_barrier((behind, ahead, across, tables))
    fids, info, columns, cosine, sine, ids, doc_rows, doc_columns = tables
    top = shift(behind[:HALF], "head", 1)
    bottom = shift(ahead[HALF:], "head", -1)
    across_near = shift(jnp.concatenate([behind, ahead]), "grp", 1)
    mine = [own, behind, ahead, top, bottom]
    across_far = shift(jnp.concatenate([top, bottom]), "grp", 1)
    theirs = [across, across_near, across_far]
    queries, message = project(fids, mine + theirs, query_key_value_weight, cosine, sine, ids)

    along, against = shift_y(message, 1), shift_y(message, -1)
    straight = shift_z(message)
    own_state, state = attend_first(queries, message, doc_rows, doc_columns)
    along = jnp.pad(along, ((0, T), (0, 0)))
    against = jnp.pad(against, ((0, MSG_ROWS - T), (0, 0)))

    def stage(s, carried):
        along, against, straight, state = carried
        next_along = shift_y(jnp.concatenate([straight, along[:T]]), 1)
        next_against = shift_y(jnp.concatenate([straight, against[T:MSG_ROWS]]), -1)
        following = shift_z(straight)
        number = jnp.full((1,), s - 1, jnp.int32)
        state = attend_stage(number, info, queries, state, along, against, straight)
        return next_along, next_against, following, state

    along, against, straight, state = lax.fori_loop(
        1, 5, stage, (along, against, straight, state)
    )
    keys = shift_y(along[:T], 1)
    values = shift_y(against[T:MSG_ROWS], -1)
    state = attend_stage(
        jnp.full((1,), 4, jnp.int32), info, queries, state, along, against, None
    )

    first, others, products = finish(
        info, queries, own_state, state, keys, values, columns, out_weight
    )
    first = shift(first, "grp", 1)
    others = shift(others, "grp", 1)

    far = (products[0] + first.astype(f32)).astype(bf16)
    far_up = shift(far[:HALF], "head", 1)
    far_down = shift(far[HALF:], "head", -1)
    up_low = (products[1, HALF:] + others[0, HALF:].astype(f32)).astype(bf16)
    down_high = (products[2, :HALF] + others[1, :HALF].astype(f32)).astype(bf16)
    up_low = shift(up_low, "head", 1)
    down_high = shift(down_high, "head", -1)
    up_high = products[1, :HALF] + others[0, :HALF].astype(f32) + far_up.astype(f32)
    down_low = products[2, HALF:] + others[1, HALF:].astype(f32) + far_down.astype(f32)
    up_high = shift(up_high.astype(bf16), "head", 1)
    down_low = shift(down_low.astype(bf16), "head", -1)
    kept = products[3] + others[2].astype(f32)
    return jnp.concatenate(
        [
            kept[:HALF] + up_high.astype(f32) + down_high.astype(f32),
            kept[HALF:] + up_low.astype(f32) + down_low.astype(f32),
        ]
    ).astype(bf16)


def solution(mesh):
    return jax.shard_map(
        body,
        mesh=mesh,
        in_specs=(
            P("tok", ("head", "grp")),
            P(("head", "grp")),
            P(None, ("head", "grp")),
            P(("head", "grp"), None),
            P("tok"),
        ),
        out_specs=P("tok", ("head", "grp")),
        check_vma=False,
    )
```
